32 devices in a mesh: gx: 2 (over core), gy: 4 (over y, x), lev: 4 (over z).
Axes of the slice: x: 2, y: 2, z: 4, core: 2. Of those that a mesh axis runs over, the one named last changes fastest.
Arguments:
- u_wind: float32 [256, 32, 512], P('lev', 'gx', 'gy'), may hold values from -6 to 6
- v_wind: float32 [256, 32, 512], P('lev', 'gx', 'gy'), may hold values from -6 to 6
- w_wind: float32 [256, 32, 512], P('lev', 'gx', 'gy'), may hold values from -4 to 4
- pressure: float32 [256, 32, 512], P('lev', 'gx', 'gy'), may hold values from -6 to 6
- buoyancy: float32 [256, 32, 512], P('lev', 'gx', 'gy'), may hold values from 0.5 to 2
- stiffness: float32 [256, 32, 512], P('lev', 'gx', 'gy'), may hold values from 0.5 to 2
Outputs:
- u_final: float32 [256, 32, 512], P('lev', 'gx', 'gy')
- v_final: float32 [256, 32, 512], P('lev', 'gx', 'gy')
- w_final: float32 [256, 32, 512], P('lev', 'gx', 'gy')
- p_final: float32 [256, 32, 512], P('lev', 'gx', 'gy')
The draws below stay inside these ranges and needn't reach their ends.
All inputs are finite; a program needn't handle non-finite values.
Results may differ from the reference program's by a relative error of at most 0.002.
Values sent between devices are 32-bit elements; how exact they have to be, the bound alone decides.
A program may use at most 128 MiB of HBM per device.

```python
import math
import jax
import jax.numpy as jnp
from jax import lax

SUBSTEPS = 3
NX = 32
NY = 512
NZ = 256


def draw_w_wind(key, part):
    walk_key, rough_key = jax.random.split(jax.random.fold_in(key, 11))
    grid_shape = (NZ, NX, NY)
    increments = jax.random.normal(walk_key, grid_shape, jnp.float32)
    random_walk = jnp.cumsum(increments, axis=0) / jnp.sqrt(jnp.float32(NZ))
    rough_part = 0.3 * jax.random.normal(rough_key, grid_shape, jnp.float32)
    return jnp.clip(random_walk + rough_part, -4.0, 4.0)


def levels(own_key, extent, cuts, least, largest):
    factor_of, own = 1.0, jax.random.fold_in(own_key, 6)
    for axis_at, blocks in cuts:
        draws = jnp.exp(jax.random.uniform(jax.random.fold_in(own, axis_at), (blocks,), jnp.float32, least / len(cuts), largest / len(cuts)))
        factor_of = factor_of * jnp.repeat(draws, extent[axis_at] // blocks).reshape([-1 if axis == axis_at else 1 for axis in range(len(extent))])
    return factor_of


def scatter_about(stream_key, dims, deviation, reach, cuts=(), kind=jnp.bfloat16):
    loudness = levels(stream_key, dims, cuts, -0.22, 0.18) if cuts else 1.0
    drawn = jax.random.normal(stream_key, dims, jnp.float32) * deviation * loudness
    return jnp.minimum(jnp.maximum(drawn, -reach), reach).astype(kind)


def setup_inputs(seed: int = 0) -> dict:
    streams_of = jax.random.split(jax.random.key(seed), 7)
    u_wind = scatter_about(streams_of[0], (NZ, NX, NY), 1.0, 6.0, ((0, 4), (1, 2), (2, 4)), jnp.float32)
    v_wind = scatter_about(streams_of[1], (NZ, NX, NY), 1.0, 6.0, ((0, 4), (1, 2), (2, 4)), jnp.float32)
    w_wind = draw_w_wind(jax.random.fold_in(streams_of[6], 71), 0)
    pressure = scatter_about(streams_of[3], (NZ, NX, NY), 1.0, 6.0, ((0, 4), (1, 2), (2, 4)), jnp.float32)
    buoyancy = jnp.clip(jnp.exp(math.log(2.0) - 1.3862944 * jax.random.uniform(streams_of[4], (NZ, NX, NY), jnp.float32) ** levels(streams_of[4], (NZ, NX, NY), ((0, 4), (1, 2), (2, 4)), -0.2, 0.2)), 0.5, 2.0)
    stiffness = jnp.clip(jnp.exp(math.log(2.0) - 1.3862944 * jax.random.uniform(streams_of[5], (NZ, NX, NY), jnp.float32) ** levels(streams_of[5], (NZ, NX, NY), ((0, 4), (1, 2), (2, 4)), -0.2, 0.2)), 0.5, 2.0)
    return dict(u_wind=u_wind, v_wind=v_wind, w_wind=w_wind, pressure=pressure, buoyancy=buoyancy, stiffness=stiffness)


courant_h = 0.3
vertical_gain = 4096.0

def neighbour(grid_field, offset, axis_number):
    return jnp.roll(grid_field, -offset, axis=axis_number)

def reference(u_wind, v_wind, w_wind, pressure, buoyancy, stiffness):
    zero_row = jnp.zeros((1,) + pressure.shape[1:], jnp.float32)
    stiff_up = jnp.concatenate([stiffness[1:], zero_row], 0)
    lower_band = -vertical_gain * buoyancy * stiffness
    lower_band = jnp.concatenate([zero_row, lower_band[1:]], 0)
    upper_band = -vertical_gain * buoyancy * stiff_up
    main_band = 1.0 + vertical_gain * buoyancy * (stiffness + stiff_up)
    lower_cols = jnp.moveaxis(lower_band, 0, -1)
    main_cols = jnp.moveaxis(main_band, 0, -1)
    upper_cols = jnp.moveaxis(upper_band, 0, -1)
    for substep in range(SUBSTEPS):
        u_new = u_wind - courant_h * buoyancy * (neighbour(pressure, 1, 1) - neighbour(pressure, -1, 1))
        v_new = v_wind - courant_h * buoyancy * (neighbour(pressure, 1, 2) - neighbour(pressure, -1, 2))
        divergence = neighbour(u_new, 1, 1) - neighbour(u_new, -1, 1) + (neighbour(v_new, 1, 2) - neighbour(v_new, -1, 2))
        p_star = pressure - courant_h * stiffness * divergence
        p_above = jnp.concatenate([p_star[1:], zero_row], 0)
        right_side = w_wind - vertical_gain * buoyancy * (p_above - p_star)
        solved = lax.linalg.tridiagonal_solve(lower_cols, main_cols, upper_cols, jnp.moveaxis(right_side, 0, -1)[..., None])
        w_new = jnp.moveaxis(solved[..., 0], -1, 0)
        w_below = jnp.concatenate([zero_row, w_new[:-1]], 0)
        pressure = p_star - stiffness * (w_new - w_below)
        u_wind, v_wind, w_wind = (u_new, v_new, w_new)
    return (u_wind, v_wind, w_wind, pressure)
```

```python
import functools

import jax
import jax.numpy as jnp
from jax import lax
from jax.experimental import pallas as pl
from jax.experimental.pallas import tpu as pltpu
from jax.sharding import PartitionSpec as P

SUBSTEPS = 3
CH = 0.3
GAIN = 4096.0
MESH = pl.DeviceIdType.MESH
GROUP = 16
F32 = jnp.float32


def kernel(
    K, nx, ny, nz,
    u_in, v_in, w_in, p_in, b_in, s_in,
    u_out, v_out, w_out, p_out,
    p, us, vs, w, s, bi, bj, E, D, H, X, Y, ps, h, uo, vo,
    i_low, i_high, i_from_up, i_from_down,
    j_own, j_from_left, j_from_right,
    hu, hbi, hv, hbj, C,
    cmine, cgath, fmine, fgath, red,
    in_sem, out_sem, hs_sem, hr_sem, cs_sem, cr_sem, ls_sem, lr_sem,
):
    gx, gy, me = lax.axis_index("gx"), lax.axis_index("gy"), lax.axis_index("lev")
    up, down = lax.rem(gx + 1, nx), lax.rem(gx + nx - 1, nx)
    right, left = lax.rem(gy + 1, ny), lax.rem(gy + ny - 1, ny)
    groups = K // GROUP
    K2, KJ = 2 * K, 8 * (K // GROUP)

    loads = []
    for n, (src, dst) in enumerate(
        ((p_in, p), (b_in, bi), (u_in, us), (v_in, vs), (s_in, s), (w_in, w))
    ):
        c = pltpu.make_async_copy(src, dst, in_sem.at[n])
        c.start()
        loads.append(c)

    barrier = pltpu.get_barrier_semaphore()
    for dev in (up, down):
        pl.semaphore_signal(barrier, inc=1, device_id={"gx": dev}, device_id_type=MESH)
    for dev in (left, right):
        pl.semaphore_signal(barrier, inc=1, device_id={"gy": dev}, device_id_type=MESH)
    for o in range(1, nz):
        pl.semaphore_signal(
            barrier, inc=1, device_id={"lev": lax.rem(me + o, nz)}, device_id_type=MESH
        )

    lane = lax.broadcasted_iota(jnp.int32, (8, 128), 1)
    sub = lax.broadcasted_iota(jnp.int32, (8, 128), 0)
    quad = lane % 4

    def roll(x, shift, axis):
        shift = shift % x.shape[axis]
        return x if shift == 0 else pltpu.roll(x, shift, axis)

    def at(ref, row, aligned=True):
        return ref[pl.ds(pl.multiple_of(row, 8) if aligned else row, 8), :]

    def put(ref, row, value):
        ref[pl.ds(pl.multiple_of(row, 8), 8), :] = value

    def each(body, carry=None, downward=False):
        def step(n, c):
            g = groups - 1 - n if downward else n
            return body(g, c)
        return lax.fori_loop(0, groups, step, carry)

    def pair(ref, g, j):
        return at(ref, g * 256 + 16 * j), at(ref, g * 256 + 16 * j + 8)

    def put_pair(ref, g, j, value):
        put(ref, g * 256 + 16 * j, value[0])
        put(ref, g * 256 + 16 * j + 8, value[1])

    def pack_edges(g, j, x, acc, ilo, ihi, f):
        row = 8 + f * K2 + g * 32 + 2 * j
        ilo[pl.ds(row, 2), :] = x[0][0:2]
        ihi[pl.ds(row, 2), :] = x[1][6:8]
        return pack_columns(j, x, acc)

    def pack_columns(j, x, acc):
        for half in range(2):
            q = 2 * j + half
            acc = jnp.where(lane // 4 == q, roll(x[half], 4 * q + 2, 1), acc)
        return acc

    zero = jnp.zeros((8, 128), F32)

    for c in loads[:4]:
        c.wait()

    def first_pack(g, carry):
        accp = accb = accv = zero
        for j in range(GROUP):
            accp = pack_edges(g, j, pair(p, g, j), accp, i_low.at[0], i_high.at[0], 0)
            xb = pair(bi, g, j)
            accb = pack_edges(g, j, xb, accb, i_low.at[0], i_high.at[0], 1)
            xu = pair(us, g, j)
            row = 8 + 2 * K2 + g * 32 + 2 * j
            i_low[0, pl.ds(row, 2), :] = xu[0][0:2]
            i_high[0, pl.ds(row, 2), :] = xu[1][6:8]
            accv = pack_columns(j, pair(vs, g, j), accv)
        j_own[0, pl.ds(pl.multiple_of(g * 8, 8), 8), :] = accp
        j_own[0, pl.ds(pl.multiple_of(KJ + g * 8, 8), 8), :] = accb
        j_own[0, pl.ds(pl.multiple_of(2 * KJ + g * 8, 8), 8), :] = accv
        return carry

    each(first_pack, 0)
    pl.semaphore_wait(barrier, 4 + nz - 1)

    def halo_copies(t):
        fields = 3 if t == 0 else 1
        ri, rj = pl.ds(8, fields * K2), pl.ds(0, fields * KJ)
        return [
            pltpu.make_async_remote_copy(
                src_ref=src.at[t, rows], dst_ref=dst.at[t, rows],
                send_sem=hs_sem.at[t, n], recv_sem=hr_sem.at[t, n],
                device_id={axis: dev}, device_id_type=MESH,
            )
            for n, (src, dst, rows, axis, dev) in enumerate((
                (j_own, j_from_left, rj, "gy", right),
                (j_own, j_from_right, rj, "gy", left),
                (i_low, i_from_up, ri, "gx", down),
                (i_high, i_from_down, ri, "gx", up),
            ))
        ]

    halos = halo_copies(0)
    for c in halos:
        c.start()

    def lev_copies(mine, gath, send, recv):
        return [
            pltpu.make_async_remote_copy(
                src_ref=mine, dst_ref=gath.at[me],
                send_sem=send.at[o - 1], recv_sem=recv.at[o - 1],
                device_id={"lev": lax.rem(me + o, nz)}, device_id_type=MESH,
            )
            for o in range(1, nz)
        ]

    loads[4].wait()

    def factor(g, carry):
        B, Z = carry
        for j in reversed(range(GROUP)):
            bb, ss = pair(bi, g, j), pair(s, g, j)
            newB, newZ = [], []
            for m in range(2):
                row = g * 256 + 16 * j + 8 * m
                gb = GAIN * bb[m]
                one = 1.0 + gb * B[m]
                d = 1.0 / (one + gb * ss[m])
                hh = gb * d
                e = hh * ss[m]
                put(D, row, d)
                put(H, row, hh)
                put(E, row, e)
                put(Y, row, hh * Z[m])
                newB.append(ss[m] * (one * d))
                newZ.append(e * Z[m])
            B, Z = tuple(newB), tuple(newZ)
        return B, Z

    one = jnp.ones((8, 128), F32)
    B, Z = each(factor, ((zero, zero), (one, one)), downward=True)

    def responses(g, carry):
        x, y = carry
        for j in range(GROUP):
            ee, hz = pair(E, g, j), pair(Y, g, j)
            x = tuple(ee[m] * x[m] for m in range(2))
            y = tuple(ee[m] * y[m] - hz[m] for m in range(2))
            put_pair(X, g, j, x)
            put_pair(Y, g, j, y)
        return x, y

    x, y = each(responses, ((one, one), (zero, zero)))
    for n, val in enumerate((x, y, Z, B)):
        for m in range(2):
            cmine[16 * n + 8 * m:16 * n + 8 * m + 8, :] = val[m]
            cgath[me, 16 * n + 8 * m:16 * n + 8 * m + 8, :] = val[m]
    consts = lev_copies(cmine, cgath, cs_sem, cr_sem)
    for c in consts:
        c.start()

    for c in halos:
        c.wait()

    def halo_rows(ref, t, f, g, j, sublane):
        return ref[t, pl.ds(8 + f * K2 + g * 32 + 2 * j - sublane, 8), :]

    def stagger(g, carry):
        rows = pl.multiple_of(g * 8, 8)
        vr = j_from_right[0, pl.ds(2 * KJ + rows, 8), :]
        br = j_from_right[0, pl.ds(KJ + rows, 8), :]
        for j in range(GROUP):
            xb, xu, xv = pair(bi, g, j), pair(us, g, j), pair(vs, g, j)
            for (val, dst, scale, f) in ((xu, us, 1.0, 2), (xb, bi, CH, 1)):
                r0, r1 = roll(val[0], 7, 0), roll(val[1], 7, 0)
                edge = halo_rows(i_from_up, 0, f, g, j, 7)
                put_pair(dst, g, j, (
                    scale * jnp.where(sub < 7, r0, r1), scale * jnp.where(sub < 7, r1, edge)
                ))
            for (val, dst, scale, packed) in ((xv, vs, 1.0, vr), (xb, bj, CH, br)):
                out = []
                for m in range(2):
                    q = 2 * j + m
                    out.append(scale * jnp.where(
                        lane == 127, roll(packed, 125 - 4 * q, 1), roll(val[m], 127, 1)
                    ))
                put_pair(dst, g, j, out)
        for r in range(4):
            row = g * 32 + 8 * r
            for (dst, f, scale) in ((hu, 2, 1.0), (hbi, 1, CH)):
                base = 8 + f * K2 + row
                below = i_from_down[0, pl.ds(base + 1, 8), :]
                own = i_low[0, pl.ds(base - 1, 8), :]
                put(dst, 8 + row, scale * jnp.where(sub % 2 == 0, below, own))
        for (dst, f, scale) in ((hv, 2, 1.0), (hbj, 1, CH)):
            fl = j_from_left[0, pl.ds(f * KJ + rows, 8), :]
            own = j_own[0, pl.ds(f * KJ + rows, 8), :]
            put(dst, rows, scale * roll(jnp.where(quad == 1, fl, own), 1, 1))
        return carry

    each(stagger, 0)

    for c in consts:
        c.wait()

    def crow(d, n):
        return cgath[d, 16 * n:16 * n + 16, :]

    beta = crow(nz - 1, 3)
    red[nz - 1, 0:16, :] = beta
    for d in range(nz - 2, -1, -1):
        R = 1.0 / (1.0 - crow(d, 1) * beta)
        zbr = crow(d, 2) * beta * R
        red[d, 16:32, :] = R
        red[d, 32:48, :] = zbr
        beta = crow(d, 3) + zbr * crow(d, 0)
        red[d, 0:16, :] = beta

    loads[5].wait()

    outs = []
    for t in range(SUBSTEPS):
        final = t == SUBSTEPS - 1
        if t > 0:
            for c in halos:
                c.wait()

        def explicit(g, A):
            rows = pl.multiple_of(g * 8, 8)
            for r in range(4):
                row = g * 32 + 8 * r
                low = i_low[t, pl.ds(pl.multiple_of(8 + row, 8), 8), :]
                below = i_from_down[t, pl.ds(pl.multiple_of(8 + row, 8), 8), :]
                put(hu, 8 + row, at(hu, 8 + row) - at(hbi, 8 + row) * (low - below))
            own = j_own[t, pl.ds(rows, 8), :]
            fl = j_from_left[t, pl.ds(rows, 8), :]
            fr = j_from_right[t, pl.ds(rows, 8), :]
            hv_new = at(hv, rows) - at(hbj, rows) * (own - roll(fl, 2, 1))
            put(hv, rows, hv_new)
            c = jnp.where(quad < 2, roll(fr, 126, 1), hv_new)
            for j in reversed(range(GROUP)):
                pp, uu, vv, ww = pair(p, g, j), pair(us, g, j), pair(vs, g, j), pair(w, g, j)
                bbi, bbj, ss = pair(bi, g, j), pair(bj, g, j), pair(s, g, j)
                ee, dd, hh = pair(E, g, j), pair(D, g, j), pair(H, g, j)
                r0, r1 = roll(pp[0], 6, 0), roll(pp[1], 6, 0)
                edge = halo_rows(i_from_up, t, 0, g, j, 6)
                pi = (jnp.where(sub < 6, r0, r1), jnp.where(sub < 6, r1, edge))
                un = tuple(uu[m] - bbi[m] * (pi[m] - pp[m]) for m in range(2))
                put_pair(us, g, j, un)
                r0, r1 = roll(un[0], 2, 0), roll(un[1], 2, 0)
                edge = at(hu, 8 + g * 32 + 2 * j, False)
                um = (jnp.where(sub < 2, edge, r0), jnp.where(sub < 2, r0, r1))
                newA, hs, pss, vn = [], [], [], []
                for m in range(2):
                    edge = roll(c, 126 - 4 * (2 * j + m), 1)
                    pj = jnp.where(lane >= 126, edge, roll(pp[m], 126, 1))
                    v_new = vv[m] - bbj[m] * (pj - pp[m])
                    vm = jnp.where(lane < 2, edge, roll(v_new, 2, 1))
                    star = pp[m] - (CH * ss[m]) * ((un[m] - um[m]) + (v_new - vm))
                    dw = dd[m] * ww[m]
                    hs.append(dw + hh[m] * (star - A[m]))
                    newA.append(ee[m] * A[m] + ((star - ee[m] * star) - ss[m] * dw))
                    pss.append(star)
                    vn.append(v_new)
                put_pair(vs, g, j, vn)
                put_pair(ps, g, j, pss)
                put_pair(h, g, j, hs)
                A = tuple(newA)
            return A

        A = each(explicit, (zero, zero), downward=True)

        def forward(g, x):
            for j in range(GROUP):
                ee, hh = pair(E, g, j), pair(h, g, j)
                x = tuple(ee[m] * x[m] + hh[m] for m in range(2))
                put_pair(w, g, j, x)
            return x

        x = each(forward, (zero, zero))
        for n, val in enumerate((A, x)):
            for m in range(2):
                fmine[t, 16 * n + 8 * m:16 * n + 8 * m + 8, :] = val[m]
                fgath[t, me, 16 * n + 8 * m:16 * n + 8 * m + 8, :] = val[m]
        sends = lev_copies(fmine.at[t], fgath.at[t], ls_sem.at[t], lr_sem.at[t])
        for c in sends:
            c.start()

        if final:
            def emit(g, carry):
                hvg = at(hv, pl.multiple_of(g * 8, 8))
                for j in range(GROUP):
                    uu, vv = pair(us, g, j), pair(vs, g, j)
                    r0, r1 = roll(uu[0], 1, 0), roll(uu[1], 1, 0)
                    edge = at(hu, 8 + g * 32 + 2 * j + 1, False)
                    put_pair(uo, g, j, (jnp.where(sub < 1, edge, r0), jnp.where(sub < 1, r0, r1)))
                    put_pair(vo, g, j, [
                        jnp.where(
                            lane == 0, roll(hvg, 125 - 4 * (2 * j + m), 1), roll(vv[m], 1, 1)
                        )
                        for m in range(2)
                    ])
                return carry

            each(emit, 0)
            for n, (src, dst) in enumerate(((uo, u_out), (vo, v_out))):
                c = pltpu.make_async_copy(src, dst, out_sem.at[n])
                c.start()
                outs.append(c)

        for c in sends:
            c.wait()

        alphas = [None] * nz
        alpha = fgath[t, nz - 1, 0:16, :]
        alphas[nz - 1] = alpha
        sums = [None] * nz
        for d in range(nz - 2, -1, -1):
            sums[d] = fgath[t, d, 16:32, :] + crow(d, 1) * alpha
            alpha = fgath[t, d, 0:16, :] + crow(d, 2) * alpha + red[d, 32:48, :] * sums[d]
            alphas[d] = alpha
        nothing = jnp.zeros((16, 128), F32)
        wb = pa = nothing
        below = nothing
        for d in range(nz):
            wb = jnp.where(me == d, below, wb)
            if d < nz - 1:
                below = red[d, 16:32, :] * (sums[d] + crow(d, 0) * below)
                above = alphas[d + 1] + red[d + 1, 0:16, :] * below
                pa = jnp.where(me == d, above, pa)
        wb2, pa2 = (wb[0:8], wb[8:16]), (pa[0:8], pa[8:16])

        def implicit(g, wprev):
            acc = zero
            for j in range(GROUP):
                w0, xx, yy = pair(w, g, j), pair(X, g, j), pair(Y, g, j)
                ss, star = pair(s, g, j), pair(ps, g, j)
                wn = tuple(w0[m] + xx[m] * wb2[m] + yy[m] * pa2[m] for m in range(2))
                pn = tuple(star[m] - ss[m] * (wn[m] - wprev[m]) for m in range(2))
                put_pair(w, g, j, wn)
                put_pair(p, g, j, pn)
                if not final:
                    acc = pack_edges(g, j, pn, acc, i_low.at[t + 1], i_high.at[t + 1], 0)
                wprev = wn
            if not final:
                j_own[t + 1, pl.ds(pl.multiple_of(g * 8, 8), 8), :] = acc
            return wprev

        each(implicit, wb2)
        if not final:
            halos = halo_copies(t + 1)
            for c in halos:
                c.start()

    for n, (src, dst) in enumerate(((w, w_out), (p, p_out))):
        c = pltpu.make_async_copy(src, dst, out_sem.at[2 + n])
        c.start()
        outs.append(c)
    for c in outs:
        c.wait()


def solution(mesh):
    nx, ny, nz = (mesh.shape[a] for a in ("gx", "gy", "lev"))

    def shards(*fields):
        K, I, J = fields[0].shape
        assert I == 16 and J == 128 and K % GROUP == 0
        R, KJ, T = K * I, 8 * (K // GROUP), SUBSTEPS
        full = pltpu.VMEM((R, J), F32)
        ihalo = pltpu.VMEM((T, 6 * K + 16, J), F32)
        jhalo = pltpu.VMEM((T, 3 * KJ, J), F32)
        outs = pl.pallas_call(
            functools.partial(kernel, K, nx, ny, nz),
            out_shape=[jax.ShapeDtypeStruct((R, J), F32)] * 4,
            in_specs=[pl.BlockSpec(memory_space=pl.ANY)] * 6,
            out_specs=[pl.BlockSpec(memory_space=pl.ANY)] * 4,
            scratch_shapes=[full] * 16 + [ihalo] * 4 + [jhalo] * 3 + [
                pltpu.VMEM((2 * K + 16, J), F32),
                pltpu.VMEM((2 * K + 16, J), F32),
                pltpu.VMEM((KJ, J), F32),
                pltpu.VMEM((KJ, J), F32),
                pltpu.VMEM((KJ, J), F32),
                pltpu.VMEM((64, J), F32),
                pltpu.VMEM((nz, 64, J), F32),
                pltpu.VMEM((T, 32, J), F32),
                pltpu.VMEM((T, nz, 32, J), F32),
                pltpu.VMEM((nz, 48, J), F32),
                pltpu.SemaphoreType.DMA((6,)),
                pltpu.SemaphoreType.DMA((4,)),
                pltpu.SemaphoreType.DMA((T, 4)),
                pltpu.SemaphoreType.DMA((T, 4)),
                pltpu.SemaphoreType.DMA((max(nz - 1, 1),)),
                pltpu.SemaphoreType.DMA((max(nz - 1, 1),)),
                pltpu.SemaphoreType.DMA((T, max(nz - 1, 1))),
                pltpu.SemaphoreType.DMA((T, max(nz - 1, 1))),
            ],
            compiler_params=pltpu.CompilerParams(collective_id=0, has_side_effects=True),
        )(*(f.reshape(R, J) for f in fields))
        return tuple(o.reshape(K, I, J) for o in outs)

    spec = P("lev", "gx", "gy")
    return jax.shard_map(
        shards, mesh=mesh, in_specs=(spec,) * 6, out_specs=(spec,) * 4, check_vma=False
    )
```

```python
import functools

import jax
import jax.numpy as jnp
from jax import lax
from jax.experimental import pallas as pl
from jax.experimental.pallas import tpu as pltpu
from jax.sharding import PartitionSpec as P

SUBSTEPS = 3
CH = 0.3
GAIN = 4096.0
MESH = pl.DeviceIdType.MESH
GROUP = 16
F32 = jnp.float32


def kernel(
    K, nx, ny, nz,
    u_in, v_in, w_in, p_in, b_in, s_in,
    uo, vo, w, p,
    us, vs, s, bi, bj, E, D, H, X, Y, ps, h,
    i_low, i_high, i_from_up, i_from_down,
    j_own, j_to_right, j_to_left, j_from_left, j_from_right,
    hu, hbi, hv, hbj, C, vbr,
    cmine, cgath, fmine, fgath, red, mine,
    in_sem, hs_sem, hr_sem, cs_sem, cr_sem, ls_sem, lr_sem,
):
    gx, gy, me = lax.axis_index("gx"), lax.axis_index("gy"), lax.axis_index("lev")
    up, down = lax.rem(gx + 1, nx), lax.rem(gx + nx - 1, nx)
    right, left = lax.rem(gy + 1, ny), lax.rem(gy + ny - 1, ny)
    groups = K // GROUP
    K2, KJ, KH = 2 * K, 8 * (K // GROUP), 4 * (K // GROUP)

    loads = []
    for n, (src, dst) in enumerate(
        ((p_in, p), (b_in, bi), (u_in, us), (v_in, vs), (s_in, s), (w_in, w))
    ):
        c = pltpu.make_async_copy(src, dst, in_sem.at[n])
        c.start()
        loads.append(c)

    barrier = pltpu.get_barrier_semaphore()
    for dev in (up, down):
        pl.semaphore_signal(barrier, inc=1, device_id={"gx": dev}, device_id_type=MESH)
    for dev in (left, right):
        pl.semaphore_signal(barrier, inc=1, device_id={"gy": dev}, device_id_type=MESH)
    for o in range(1, nz):
        pl.semaphore_signal(
            barrier, inc=1, device_id={"lev": lax.rem(me + o, nz)}, device_id_type=MESH
        )

    lane = lax.broadcasted_iota(jnp.int32, (8, 128), 1)
    sub = lax.broadcasted_iota(jnp.int32, (8, 128), 0)
    quad = lane % 4

    def roll(x, shift, axis):
        shift = shift % x.shape[axis]
        return x if shift == 0 else pltpu.roll(x, shift, axis)

    def at(ref, row, aligned=True):
        return ref[pl.ds(pl.multiple_of(row, 8) if aligned else row, 8), :]

    def put(ref, row, value):
        ref[pl.ds(pl.multiple_of(row, 8), 8), :] = value

    def each(body, carry=None, downward=False):
        def step(n, c):
            g = groups - 1 - n if downward else n
            return body(g, c)
        return lax.fori_loop(0, groups, step, carry)

    def pair(ref, g, j):
        return at(ref, g * 256 + 16 * j), at(ref, g * 256 + 16 * j + 8)

    def put_pair(ref, g, j, value):
        put(ref, g * 256 + 16 * j, value[0])
        put(ref, g * 256 + 16 * j + 8, value[1])

    def pack_edges(g, j, x, acc, ilo, ihi, f):
        row = 8 + f * K2 + g * 32 + 2 * j
        ilo[pl.ds(row, 2), :] = x[0][0:2]
        ihi[pl.ds(row, 2), :] = x[1][6:8]
        return pack_columns(j, x, acc)

    def pack_columns(j, x, acc):
        for half in range(2):
            q = 2 * j + half
            acc = jnp.where(lane // 4 == q, roll(x[half], 4 * q + 2, 1), acc)
        return acc

    zero = jnp.zeros((8, 128), F32)

    for c in loads[:4]:
        c.wait()

    def first_pack(g, carry):
        accp = accb = accv = zero
        for j in range(GROUP):
            accp = pack_edges(g, j, pair(p, g, j), accp, i_low.at[0], i_high.at[0], 0)
            xb = pair(bi, g, j)
            accb = pack_edges(g, j, xb, accb, i_low.at[0], i_high.at[0], 1)
            xu = pair(us, g, j)
            row = 8 + 2 * K2 + g * 32 + 2 * j
            i_low[0, pl.ds(row, 2), :] = xu[0][0:2]
            i_high[0, pl.ds(row, 2), :] = xu[1][6:8]
            accv = pack_columns(j, pair(vs, g, j), accv)
        j_own[0, pl.ds(pl.multiple_of(g * 8, 8), 8), :] = accp
        j_own[0, pl.ds(pl.multiple_of(KJ + g * 8, 8), 8), :] = accb
        j_own[0, pl.ds(pl.multiple_of(2 * KJ + g * 8, 8), 8), :] = accv
        return carry

    each(first_pack, 0)

    def dense(t, f):
        for n in range(groups // 2):
            a, b = (j_own[t, 16 * n + 8 * m:16 * n + 8 * m + 8, :] for m in range(2))
            j_to_right[t, 8 * n:8 * n + 8, :] = jnp.where(quad < 2, a, roll(b, 2, 1))
            j_to_left[t, 8 * n:8 * n + 8, :] = jnp.where(quad < 2, roll(a, -2, 1), b)
            if f:
                rights, lefts = [], []
                for m in range(2):
                    k = 16 * n + 8 * m
                    ab = j_own[t, KJ + k:KJ + k + 8, :]
                    av = j_own[t, 2 * KJ + k:2 * KJ + k + 8, :]
                    rights.append(jnp.where(quad == 0, roll(av, -1, 1), ab))
                    lefts.append(jnp.where(quad == 0, roll(av, -2, 1), roll(ab, -1, 1)))
                k = KH + 8 * n
                for ref, (a, b) in ((j_to_right, rights), (j_to_left, lefts)):
                    ref[t, k:k + 8, :] = jnp.where(quad < 2, a, roll(b, 2, 1))

    dense(0, True)
    pl.semaphore_wait(barrier, 4 + nz - 1)

    def halo_copies(t):
        ri = pl.ds(8, (3 if t == 0 else 1) * K2)
        rj = pl.ds(0, (2 if t == 0 else 1) * KH)
        return [
            pltpu.make_async_remote_copy(
                src_ref=src.at[t, rows], dst_ref=dst.at[t, rows],
                send_sem=hs_sem.at[t, n], recv_sem=hr_sem.at[t, n],
                device_id={axis: dev}, device_id_type=MESH,
            )
            for n, (src, dst, rows, axis, dev) in enumerate((
                (j_to_right, j_from_left, rj, "gy", right),
                (j_to_left, j_from_right, rj, "gy", left),
                (i_low, i_from_up, ri, "gx", down),
                (i_high, i_from_down, ri, "gx", up),
            ))
        ]

    halos = halo_copies(0)
    for c in halos:
        c.start()

    def lev_copies(src, gath, send, recv):
        return [
            pltpu.make_async_remote_copy(
                src_ref=src(lax.div(me + o, nz)), dst_ref=gath.at[me],
                send_sem=send.at[o - 1], recv_sem=recv.at[o - 1],
                device_id={"lev": lax.rem(me + o, nz)}, device_id_type=MESH,
            )
            for o in range(1, nz)
        ]

    loads[4].wait()

    def factor(g, carry):
        B, Z = carry
        for j in reversed(range(GROUP)):
            bb, ss = pair(bi, g, j), pair(s, g, j)
            newB, newZ = [], []
            for m in range(2):
                row = g * 256 + 16 * j + 8 * m
                gb = GAIN * bb[m]
                one = 1.0 + gb * B[m]
                d = 1.0 / (one + gb * ss[m])
                hh = gb * d
                e = hh * ss[m]
                put(D, row, d)
                put(H, row, hh)
                put(E, row, e)
                put(Y, row, hh * Z[m])
                newB.append(ss[m] * (one * d))
                newZ.append(e * Z[m])
            B, Z = tuple(newB), tuple(newZ)
        return B, Z

    one = jnp.ones((8, 128), F32)
    B, Z = each(factor, ((zero, zero), (one, one)), downward=True)

    def responses(g, carry):
        x, y = carry
        for j in range(GROUP):
            ee, hz = pair(E, g, j), pair(Y, g, j)
            x = tuple(ee[m] * x[m] for m in range(2))
            y = tuple(ee[m] * y[m] - hz[m] for m in range(2))
            put_pair(X, g, j, x)
            put_pair(Y, g, j, y)
        return x, y

    x, y = each(responses, ((one, one), (zero, zero)))
    for n, val in enumerate((x, y, Z, B)):
        for m in range(2):
            cmine[16 * n + 8 * m:16 * n + 8 * m + 8, :] = val[m]
            cgath[me, 16 * n + 8 * m:16 * n + 8 * m + 8, :] = val[m]
    consts = lev_copies(lambda below: cmine, cgath, cs_sem, cr_sem)
    for c in consts:
        c.start()

    def crow(d, n):
        return cgath[d, 16 * n:16 * n + 16, :]

    for c in halos:
        c.wait()

    def halo_rows(ref, t, f, g, j, sublane):
        return ref[t, pl.ds(8 + f * K2 + g * 32 + 2 * j - sublane, 8), :]

    for n in range(groups // 2):
        fr = j_from_right[0, KH + 8 * n:KH + 8 * n + 8, :]
        fl = j_from_left[0, KH + 8 * n:KH + 8 * n + 8, :]
        for m in range(2):
            k = 16 * n + 8 * m
            vbr[k:k + 8, :] = roll(fr, -2 * m, 1)
            flg = roll(fl, -2 * m, 1)
            ab = j_own[0, KJ + k:KJ + k + 8, :]
            av = j_own[0, 2 * KJ + k:2 * KJ + k + 8, :]
            hv[k:k + 8, :] = jnp.where(quad == 2, roll(flg, 2, 1), roll(av, 1, 1))
            hbj[k:k + 8, :] = CH * roll(jnp.where(quad == 1, flg, ab), 1, 1)

    def stagger(g, carry):
        packed = at(vbr, g * 8)
        for j in range(GROUP):
            xb, xu, xv = pair(bi, g, j), pair(us, g, j), pair(vs, g, j)
            for (val, dst, scale, f) in ((xu, us, 1.0, 2), (xb, bi, CH, 1)):
                r0, r1 = roll(val[0], 7, 0), roll(val[1], 7, 0)
                edge = halo_rows(i_from_up, 0, f, g, j, 7)
                put_pair(dst, g, j, (
                    scale * jnp.where(sub < 7, r0, r1), scale * jnp.where(sub < 7, r1, edge)
                ))
            for (val, dst, scale, first) in ((xv, vs, 1.0, 127), (xb, bj, CH, 126)):
                out = []
                for m in range(2):
                    q = 2 * j + m
                    out.append(scale * jnp.where(
                        lane == 127, roll(packed, first - 4 * q, 1), roll(val[m], 127, 1)
                    ))
                put_pair(dst, g, j, out)
        for r in range(4):
            row = g * 32 + 8 * r
            for (dst, f, scale) in ((hu, 2, 1.0), (hbi, 1, CH)):
                base = 8 + f * K2 + row
                below = i_from_down[0, pl.ds(base + 1, 8), :]
                own = i_low[0, pl.ds(base - 1, 8), :]
                put(dst, 8 + row, scale * jnp.where(sub % 2 == 0, below, own))
        return carry

    each(stagger, 0)

    loads[5].wait()

    for t in range(SUBSTEPS):
        final = t == SUBSTEPS - 1
        if t > 0:
            for c in halos:
                c.wait()

        for n in range(groups // 2):
            fr = j_from_right[t, 8 * n:8 * n + 8, :]
            fl = j_from_left[t, 8 * n:8 * n + 8, :]
            for m in range(2):
                k = 16 * n + 8 * m
                before = roll(fl, 2, 1) if m == 0 else fl
                own = j_own[t, k:k + 8, :]
                hv_new = hv[k:k + 8, :] - hbj[k:k + 8, :] * (own - before)
                hv[k:k + 8, :] = hv_new
                C[k:k + 8, :] = jnp.where(quad < 2, roll(fr, -2 * m, 1), hv_new)

        def explicit(g, A):
            for r in range(4):
                row = g * 32 + 8 * r
                low = i_low[t, pl.ds(pl.multiple_of(8 + row, 8), 8), :]
                below = i_from_down[t, pl.ds(pl.multiple_of(8 + row, 8), 8), :]
                put(hu, 8 + row, at(hu, 8 + row) - at(hbi, 8 + row) * (low - below))
            c = at(C, g * 8)
            for j in reversed(range(GROUP)):
                pp, uu, vv, ww = pair(p, g, j), pair(us, g, j), pair(vs, g, j), pair(w, g, j)
                bbi, bbj, ss = pair(bi, g, j), pair(bj, g, j), pair(s, g, j)
                ee, dd, hh = pair(E, g, j), pair(D, g, j), pair(H, g, j)
                r0, r1 = roll(pp[0], 6, 0), roll(pp[1], 6, 0)
                edge = halo_rows(i_from_up, t, 0, g, j, 6)
                pi = (jnp.where(sub < 6, r0, r1), jnp.where(sub < 6, r1, edge))
                un = tuple(uu[m] - bbi[m] * (pi[m] - pp[m]) for m in range(2))
                put_pair(us, g, j, un)
                r0, r1 = roll(un[0], 2, 0), roll(un[1], 2, 0)
                edge = at(hu, 8 + g * 32 + 2 * j, False)
                um = (jnp.where(sub < 2, edge, r0), jnp.where(sub < 2, r0, r1))
                newA, hs, pss, vn = [], [], [], []
                for m in range(2):
                    edge = roll(c, 126 - 4 * (2 * j + m), 1)
                    pj = jnp.where(lane >= 126, edge, roll(pp[m], 126, 1))
                    v_new = vv[m] - bbj[m] * (pj - pp[m])
                    vm = jnp.where(lane < 2, edge, roll(v_new, 2, 1))
                    star = pp[m] - (CH * ss[m]) * ((un[m] - um[m]) + (v_new - vm))
                    dw = dd[m] * ww[m]
                    hs.append(dw + hh[m] * (star - A[m]))
                    newA.append(ee[m] * A[m] + ((star - ee[m] * star) - ss[m] * dw))
                    pss.append(star)
                    vn.append(v_new)
                put_pair(vs, g, j, vn)
                put_pair(ps, g, j, pss)
                put_pair(h, g, j, hs)
                A = tuple(newA)
            return A

        A = each(explicit, (zero, zero), downward=True)

        def forward(g, x):
            for j in range(GROUP):
                ee, hh = pair(E, g, j), pair(h, g, j)
                x = tuple(ee[m] * x[m] + hh[m] for m in range(2))
                put_pair(w, g, j, x)
            return x

        x = each(forward, (zero, zero))
        if t == 0:
            for c in consts:
                c.wait()
            nothing = jnp.zeros((16, 128), F32)
            picks = {name: nothing for name in ("psi", "r2", "beta", "r", "wa", "aw", "lam")}

            def pick(name, d, val):
                picks[name] = jnp.where(me == d, val, picks[name])

            beta = nothing
            betas = [None] * nz
            for d in range(nz - 1, -1, -1):
                R = 1.0 / (1.0 - crow(d, 1) * beta)
                zbr = crow(d, 2) * beta * R
                lam = crow(d, 2) + zbr * crow(d, 1)
                red[d, 0:16, :] = lam
                for name, val in (("beta", beta), ("r", R), ("aw", zbr), ("lam", lam)):
                    pick(name, d, val)
                beta = crow(d, 3) + zbr * crow(d, 0)
                betas[d] = beta
            psi = nothing
            for d in range(nz):
                xr = crow(d, 0) / (1.0 - psi * crow(d, 3))
                xrp = xr * psi
                red[d, 16:32, :] = xr
                pick("psi", d, psi)
                pick("r2", d, 1.0 / (1.0 - psi * betas[d]))
                pick("wa", d, xrp)
                psi = crow(d, 1) + xrp * crow(d, 2)
            for n, name in enumerate(picks):
                mine[16 * n:16 * n + 16, :] = picks[name]

        psi, r2, beta, r, wa, aw, lam = (mine[16 * n:16 * n + 16, :] for n in range(7))
        A0, W0 = (jnp.concatenate(q, 0) for q in (A, x))
        up_row, down_row = W0 + wa * A0, A0 + aw * W0
        fmine[t, 0], fmine[t, 1] = up_row, down_row
        sends = lev_copies(lambda below: fmine.at[t, below], fgath.at[t], ls_sem.at[t], lr_sem.at[t])
        for c in sends:
            c.start()

        if final:
            def emit(g, carry):
                hvg = at(hv, pl.multiple_of(g * 8, 8))
                for j in range(GROUP):
                    uu, vv = pair(us, g, j), pair(vs, g, j)
                    r0, r1 = roll(uu[0], 1, 0), roll(uu[1], 1, 0)
                    edge = at(hu, 8 + g * 32 + 2 * j + 1, False)
                    put_pair(uo, g, j, (jnp.where(sub < 1, edge, r0), jnp.where(sub < 1, r0, r1)))
                    put_pair(vo, g, j, [
                        jnp.where(
                            lane == 0, roll(hvg, 125 - 4 * (2 * j + m), 1), roll(vv[m], 1, 1)
                        )
                        for m in range(2)
                    ])
                return carry

            each(emit, 0)
        for c in sends:
            c.wait()

        omega = alpha = jnp.zeros((16, 128), F32)
        for d in range(nz - 1):
            omega = jnp.where(me > d, fgath[t, d] + red[d, 16:32, :] * omega, omega)
        for d in range(nz - 1, 0, -1):
            alpha = jnp.where(me < d, fgath[t, d] + red[d, 0:16, :] * alpha, alpha)
        wb = r2 * (omega + psi * (down_row + lam * alpha))
        pa = alpha + beta * (r * (W0 + crow(me, 1) * alpha + crow(me, 0) * wb))
        wb2, pa2 = (wb[0:8], wb[8:16]), (pa[0:8], pa[8:16])

        def implicit(g, wprev):
            acc = zero
            for j in range(GROUP):
                w0, xx, yy = pair(w, g, j), pair(X, g, j), pair(Y, g, j)
                ss, star = pair(s, g, j), pair(ps, g, j)
                wn = tuple(w0[m] + xx[m] * wb2[m] + yy[m] * pa2[m] for m in range(2))
                pn = tuple(star[m] - ss[m] * (wn[m] - wprev[m]) for m in range(2))
                put_pair(w, g, j, wn)
                put_pair(p, g, j, pn)
                if not final:
                    acc = pack_edges(g, j, pn, acc, i_low.at[t + 1], i_high.at[t + 1], 0)
                wprev = wn
            if not final:
                j_own[t + 1, pl.ds(pl.multiple_of(g * 8, 8), 8), :] = acc
            return wprev

        each(implicit, wb2)
        if not final:
            dense(t + 1, False)
            halos = halo_copies(t + 1)
            for c in halos:
                c.start()


def store(u, v, w, p, u_out, v_out, w_out, p_out, sem):
    copies = [
        pltpu.make_async_copy(src, dst, sem.at[n])
        for n, (src, dst) in enumerate(((u, u_out), (v, v_out), (w, w_out), (p, p_out)))
    ]
    for c in copies:
        c.start()
    for c in copies:
        c.wait()


def solution(mesh):
    nx, ny, nz = (mesh.shape[a] for a in ("gx", "gy", "lev"))

    def shards(*fields):
        K, I, J = fields[0].shape
        assert I == 16 and J == 128 and K % (2 * GROUP) == 0
        R, KJ, T = K * I, 8 * (K // GROUP), SUBSTEPS
        full = pltpu.VMEM((R, J), F32)
        ihalo = pltpu.VMEM((T, 6 * K + 16, J), F32)
        jhalo = pltpu.VMEM((T, 3 * KJ, J), F32)
        jdense = pltpu.VMEM((T, KJ, J), F32)
        outs = pl.pallas_call(
            functools.partial(kernel, K, nx, ny, nz),
            out_shape=[full] * 4,
            in_specs=[pl.BlockSpec(memory_space=pl.ANY)] * 6,
            out_specs=[pl.BlockSpec(memory_space=pltpu.VMEM)] * 4,
            scratch_shapes=[full] * 12 + [ihalo] * 4 + [jhalo] + [jdense] * 4 + [
                pltpu.VMEM((2 * K + 16, J), F32),
                pltpu.VMEM((2 * K + 16, J), F32),
                pltpu.VMEM((KJ, J), F32),
                pltpu.VMEM((KJ, J), F32),
                pltpu.VMEM((KJ, J), F32),
                pltpu.VMEM((KJ, J), F32),
                pltpu.VMEM((64, J), F32),
                pltpu.VMEM((nz, 64, J), F32),
                pltpu.VMEM((T, 2, 16, J), F32),
                pltpu.VMEM((T, nz, 16, J), F32),
                pltpu.VMEM((nz, 32, J), F32),
                pltpu.VMEM((112, J), F32),
                pltpu.SemaphoreType.DMA((6,)),
                pltpu.SemaphoreType.DMA((T, 4)),
                pltpu.SemaphoreType.DMA((T, 4)),
                pltpu.SemaphoreType.DMA((max(nz - 1, 1),)),
                pltpu.SemaphoreType.DMA((max(nz - 1, 1),)),
                pltpu.SemaphoreType.DMA((T, max(nz - 1, 1))),
                pltpu.SemaphoreType.DMA((T, max(nz - 1, 1))),
            ],
            compiler_params=pltpu.CompilerParams(collective_id=0, has_side_effects=True),
        )(*(f.reshape(R, J) for f in fields))
        outs = pl.pallas_call(
            store,
            out_shape=[jax.ShapeDtypeStruct((R, J), F32)] * 4,
            in_specs=[pl.BlockSpec(memory_space=pltpu.VMEM)] * 4,
            out_specs=[pl.BlockSpec(memory_space=pl.ANY)] * 4,
            scratch_shapes=[pltpu.SemaphoreType.DMA((4,))],
        )(*(pltpu.with_memory_space_constraint(o, pltpu.VMEM) for o in outs))
        return tuple(o.reshape(K, I, J) for o in outs)

    spec = P("lev", "gx", "gy")
    return jax.shard_map(
        shards, mesh=mesh, in_specs=(spec,) * 6, out_specs=(spec,) * 4, check_vma=False
    )
```

```python
import functools

import jax
import jax.numpy as jnp
from jax import lax
from jax.experimental import pallas as pl
from jax.experimental.pallas import tpu as pltpu
from jax.sharding import PartitionSpec as P

SUBSTEPS = 3
CH = 0.3
GAIN = 4096.0
MESH = pl.DeviceIdType.MESH
GROUP = 16
F32 = jnp.float32


def kernel(
    K, nx, ny, nz,
    u_in, v_in, w_in, p_in, b_in, s_in,
    uo, vo, w, ps, X, Y, s, ends,
    p, us, vs, bi, bj, E, D, H, h,
    i_low, i_high, i_from_up, i_from_down,
    j_own, j_to_right, j_to_left, j_from_left, j_from_right,
    hu, hbi, hv, hbj, C, vbr,
    cmine, cgath, fmine, fgath, red, mine,
    in_sem, hs_sem, hr_sem, cs_sem, cr_sem, ls_sem, lr_sem,
):
    gx, gy, me = lax.axis_index("gx"), lax.axis_index("gy"), lax.axis_index("lev")
    up, down = lax.rem(gx + 1, nx), lax.rem(gx + nx - 1, nx)
    right, left = lax.rem(gy + 1, ny), lax.rem(gy + ny - 1, ny)
    groups = K // GROUP
    K2, KJ, KH = 2 * K, 8 * (K // GROUP), 4 * (K // GROUP)

    loads = []
    for n, (src, dst) in enumerate(
        ((p_in, p), (b_in, bi), (u_in, us), (v_in, vs), (s_in, s), (w_in, w))
    ):
        c = pltpu.make_async_copy(src, dst, in_sem.at[n])
        c.start()
        loads.append(c)

    barrier = pltpu.get_barrier_semaphore()
    for dev in (up, down):
        pl.semaphore_signal(barrier, inc=1, device_id={"gx": dev}, device_id_type=MESH)
    for dev in (left, right):
        pl.semaphore_signal(barrier, inc=1, device_id={"gy": dev}, device_id_type=MESH)
    for o in range(1, nz):
        pl.semaphore_signal(
            barrier, inc=1, device_id={"lev": lax.rem(me + o, nz)}, device_id_type=MESH
        )

    lane = lax.broadcasted_iota(jnp.int32, (8, 128), 1)
    sub = lax.broadcasted_iota(jnp.int32, (8, 128), 0)
    quad = lane % 4

    def roll(x, shift, axis):
        shift = shift % x.shape[axis]
        return x if shift == 0 else pltpu.roll(x, shift, axis)

    def at(ref, row, aligned=True):
        return ref[pl.ds(pl.multiple_of(row, 8) if aligned else row, 8), :]

    def put(ref, row, value):
        ref[pl.ds(pl.multiple_of(row, 8), 8), :] = value

    def each(body, carry=None, downward=False):
        def step(n, c):
            g = groups - 1 - n if downward else n
            return body(g, c)
        return lax.fori_loop(0, groups, step, carry)

    def pair(ref, g, j):
        return at(ref, g * 256 + 16 * j), at(ref, g * 256 + 16 * j + 8)

    def put_pair(ref, g, j, value):
        put(ref, g * 256 + 16 * j, value[0])
        put(ref, g * 256 + 16 * j + 8, value[1])

    def pack_edges(g, j, x, acc, ilo, ihi, f):
        row = 8 + f * K2 + g * 32 + 2 * j
        ilo[pl.ds(row, 2), :] = x[0][0:2]
        ihi[pl.ds(row, 2), :] = x[1][6:8]
        return pack_columns(j, x, acc)

    def pack_columns(j, x, acc):
        for half in range(2):
            q = 2 * j + half
            acc = jnp.where(lane // 4 == q, roll(x[half], 4 * q + 2, 1), acc)
        return acc

    zero = jnp.zeros((8, 128), F32)

    for c in loads[:4]:
        c.wait()

    def first_pack(g, carry):
        accp = accb = accv = zero
        for j in range(GROUP):
            accp = pack_edges(g, j, pair(p, g, j), accp, i_low.at[0], i_high.at[0], 0)
            xb = pair(bi, g, j)
            accb = pack_edges(g, j, xb, accb, i_low.at[0], i_high.at[0], 1)
            xu = pair(us, g, j)
            row = 8 + 2 * K2 + g * 32 + 2 * j
            i_low[0, pl.ds(row, 2), :] = xu[0][0:2]
            i_high[0, pl.ds(row, 2), :] = xu[1][6:8]
            accv = pack_columns(j, pair(vs, g, j), accv)
        j_own[0, pl.ds(pl.multiple_of(g * 8, 8), 8), :] = accp
        j_own[0, pl.ds(pl.multiple_of(KJ + g * 8, 8), 8), :] = accb
        j_own[0, pl.ds(pl.multiple_of(2 * KJ + g * 8, 8), 8), :] = accv
        return carry

    each(first_pack, 0)

    def dense(t, f):
        for n in range(groups // 2):
            a, b = (j_own[t, 16 * n + 8 * m:16 * n + 8 * m + 8, :] for m in range(2))
            j_to_right[t, 8 * n:8 * n + 8, :] = jnp.where(quad < 2, a, roll(b, 2, 1))
            j_to_left[t, 8 * n:8 * n + 8, :] = jnp.where(quad < 2, roll(a, -2, 1), b)
            if f:
                rights, lefts = [], []
                for m in range(2):
                    k = 16 * n + 8 * m
                    ab = j_own[t, KJ + k:KJ + k + 8, :]
                    av = j_own[t, 2 * KJ + k:2 * KJ + k + 8, :]
                    rights.append(jnp.where(quad == 0, roll(av, -1, 1), ab))
                    lefts.append(jnp.where(quad == 0, roll(av, -2, 1), roll(ab, -1, 1)))
                k = KH + 8 * n
                for ref, (a, b) in ((j_to_right, rights), (j_to_left, lefts)):
                    ref[t, k:k + 8, :] = jnp.where(quad < 2, a, roll(b, 2, 1))

    dense(0, True)
    pl.semaphore_wait(barrier, 4 + nz - 1)

    def halo_copies(t):
        ri = pl.ds(8, (3 if t == 0 else 1) * K2)
        rj = pl.ds(0, (2 if t == 0 else 1) * KH)
        return [
            pltpu.make_async_remote_copy(
                src_ref=src.at[t, rows], dst_ref=dst.at[t, rows],
                send_sem=hs_sem.at[t, n], recv_sem=hr_sem.at[t, n],
                device_id={axis: dev}, device_id_type=MESH,
            )
            for n, (src, dst, rows, axis, dev) in enumerate((
                (j_to_right, j_from_left, rj, "gy", right),
                (j_to_left, j_from_right, rj, "gy", left),
                (i_low, i_from_up, ri, "gx", down),
                (i_high, i_from_down, ri, "gx", up),
            ))
        ]

    halos = halo_copies(0)
    for c in halos:
        c.start()

    def lev_copies(src, gath, send, recv):
        return [
            pltpu.make_async_remote_copy(
                src_ref=src(lax.div(me + o, nz)), dst_ref=gath.at[me],
                send_sem=send.at[o - 1], recv_sem=recv.at[o - 1],
                device_id={"lev": lax.rem(me + o, nz)}, device_id_type=MESH,
            )
            for o in range(1, nz)
        ]

    loads[4].wait()

    def factor(g, carry):
        B, Z = carry
        for j in reversed(range(GROUP)):
            bb, ss = pair(bi, g, j), pair(s, g, j)
            newB, newZ = [], []
            for m in range(2):
                row = g * 256 + 16 * j + 8 * m
                gb = GAIN * bb[m]
                one = 1.0 + gb * B[m]
                d = 1.0 / (one + gb * ss[m])
                hh = gb * d
                e = hh * ss[m]
                put(D, row, d)
                put(H, row, hh)
                put(E, row, e)
                put(Y, row, hh * Z[m])
                newB.append(ss[m] * (one * d))
                newZ.append(e * Z[m])
            B, Z = tuple(newB), tuple(newZ)
        return B, Z

    one = jnp.ones((8, 128), F32)
    B, Z = each(factor, ((zero, zero), (one, one)), downward=True)

    def responses(g, carry):
        x, y = carry
        for j in range(GROUP):
            ee, hz = pair(E, g, j), pair(Y, g, j)
            x = tuple(ee[m] * x[m] for m in range(2))
            y = tuple(ee[m] * y[m] - hz[m] for m in range(2))
            put_pair(X, g, j, x)
            put_pair(Y, g, j, y)
        return x, y

    x, y = each(responses, ((one, one), (zero, zero)))
    for n, val in enumerate((x, y, B)):
        for m in range(2):
            cmine[16 * n + 8 * m:16 * n + 8 * m + 8, :] = val[m]
            cgath[me, 16 * n + 8 * m:16 * n + 8 * m + 8, :] = val[m]
    consts = lev_copies(lambda below: cmine, cgath, cs_sem, cr_sem)
    for c in consts:
        c.start()

    def crow(d, n):
        return cgath[d, 16 * n:16 * n + 16, :]

    for c in halos:
        c.wait()

    def halo_rows(ref, t, f, g, j, sublane):
        return ref[t, pl.ds(8 + f * K2 + g * 32 + 2 * j - sublane, 8), :]

    for n in range(groups // 2):
        fr = j_from_right[0, KH + 8 * n:KH + 8 * n + 8, :]
        fl = j_from_left[0, KH + 8 * n:KH + 8 * n + 8, :]
        for m in range(2):
            k = 16 * n + 8 * m
            vbr[k:k + 8, :] = roll(fr, -2 * m, 1)
            flg = roll(fl, -2 * m, 1)
            ab = j_own[0, KJ + k:KJ + k + 8, :]
            av = j_own[0, 2 * KJ + k:2 * KJ + k + 8, :]
            hv[k:k + 8, :] = jnp.where(quad == 2, roll(flg, 2, 1), roll(av, 1, 1))
            hbj[k:k + 8, :] = CH * roll(jnp.where(quad == 1, flg, ab), 1, 1)

    def stagger(g, carry):
        packed = at(vbr, g * 8)
        for j in range(GROUP):
            xb, xu, xv = pair(bi, g, j), pair(us, g, j), pair(vs, g, j)
            for (val, dst, scale, f) in ((xu, us, 1.0, 2), (xb, bi, CH, 1)):
                r0, r1 = roll(val[0], 7, 0), roll(val[1], 7, 0)
                edge = halo_rows(i_from_up, 0, f, g, j, 7)
                put_pair(dst, g, j, (
                    scale * jnp.where(sub < 7, r0, r1), scale * jnp.where(sub < 7, r1, edge)
                ))
            for (val, dst, scale, first) in ((xv, vs, 1.0, 127), (xb, bj, CH, 126)):
                out = []
                for m in range(2):
                    q = 2 * j + m
                    out.append(scale * jnp.where(
                        lane == 127, roll(packed, first - 4 * q, 1), roll(val[m], 127, 1)
                    ))
                put_pair(dst, g, j, out)
        for r in range(4):
            row = g * 32 + 8 * r
            for (dst, f, scale) in ((hu, 2, 1.0), (hbi, 1, CH)):
                base = 8 + f * K2 + row
                below = i_from_down[0, pl.ds(base + 1, 8), :]
                own = i_low[0, pl.ds(base - 1, 8), :]
                put(dst, 8 + row, scale * jnp.where(sub % 2 == 0, below, own))
        return carry

    each(stagger, 0)

    loads[5].wait()

    for t in range(SUBSTEPS):
        final = t == SUBSTEPS - 1
        if t > 0:
            for c in halos:
                c.wait()

        for n in range(groups // 2):
            fr = j_from_right[t, 8 * n:8 * n + 8, :]
            fl = j_from_left[t, 8 * n:8 * n + 8, :]
            for m in range(2):
                k = 16 * n + 8 * m
                before = roll(fl, 2, 1) if m == 0 else fl
                own = j_own[t, k:k + 8, :]
                hv_new = hv[k:k + 8, :] - hbj[k:k + 8, :] * (own - before)
                hv[k:k + 8, :] = hv_new
                C[k:k + 8, :] = jnp.where(quad < 2, roll(fr, -2 * m, 1), hv_new)

        def explicit(g, A):
            for r in range(4):
                row = g * 32 + 8 * r
                low = i_low[t, pl.ds(pl.multiple_of(8 + row, 8), 8), :]
                below = i_from_down[t, pl.ds(pl.multiple_of(8 + row, 8), 8), :]
                put(hu, 8 + row, at(hu, 8 + row) - at(hbi, 8 + row) * (low - below))
            c = at(C, g * 8)
            for j in reversed(range(GROUP)):
                pp, uu, vv, ww = pair(p, g, j), pair(us, g, j), pair(vs, g, j), pair(w, g, j)
                bbi, bbj, ss = pair(bi, g, j), pair(bj, g, j), pair(s, g, j)
                ee, dd, hh = pair(E, g, j), pair(D, g, j), pair(H, g, j)
                r0, r1 = roll(pp[0], 6, 0), roll(pp[1], 6, 0)
                edge = halo_rows(i_from_up, t, 0, g, j, 6)
                pi = (jnp.where(sub < 6, r0, r1), jnp.where(sub < 6, r1, edge))
                un = tuple(uu[m] - bbi[m] * (pi[m] - pp[m]) for m in range(2))
                put_pair(us, g, j, un)
                r0, r1 = roll(un[0], 2, 0), roll(un[1], 2, 0)
                edge = at(hu, 8 + g * 32 + 2 * j, False)
                um = (jnp.where(sub < 2, edge, r0), jnp.where(sub < 2, r0, r1))
                newA, hs, pss, vn = [], [], [], []
                for m in range(2):
                    edge = roll(c, 126 - 4 * (2 * j + m), 1)
                    pj = jnp.where(lane >= 126, edge, roll(pp[m], 126, 1))
                    v_new = vv[m] - bbj[m] * (pj - pp[m])
                    vm = jnp.where(lane < 2, edge, roll(v_new, 2, 1))
                    star = pp[m] - (CH * ss[m]) * ((un[m] - um[m]) + (v_new - vm))
                    dw = dd[m] * ww[m]
                    hs.append(dw + hh[m] * (star - A[m]))
                    newA.append(ee[m] * A[m] + ((star - ee[m] * star) - ss[m] * dw))
                    pss.append(star)
                    vn.append(v_new)
                put_pair(vs, g, j, vn)
                put_pair(ps, g, j, pss)
                put_pair(h, g, j, hs)
                A = tuple(newA)
            return A

        A = each(explicit, (zero, zero), downward=True)

        def forward(g, x):
            for j in range(GROUP):
                ee, hh = pair(E, g, j), pair(h, g, j)
                x = tuple(ee[m] * x[m] + hh[m] for m in range(2))
                put_pair(w, g, j, x)
            return x

        x = each(forward, (zero, zero))
        if t == 0:
            for c in consts:
                c.wait()
            nothing = jnp.zeros((16, 128), F32)
            picks = {name: nothing for name in ("psi", "r2", "beta", "r", "wa", "aw", "lam")}

            def pick(name, d, val):
                picks[name] = jnp.where(me == d, val, picks[name])

            beta = nothing
            betas = [None] * nz
            for d in range(nz - 1, -1, -1):
                R = 1.0 / (1.0 - crow(d, 1) * beta)
                zbr = crow(d, 0) * beta * R
                lam = crow(d, 0) + zbr * crow(d, 1)
                red[d, 0:16, :] = lam
                for name, val in (("beta", beta), ("r", R), ("aw", zbr), ("lam", lam)):
                    pick(name, d, val)
                beta = crow(d, 2) + zbr * crow(d, 0)
                betas[d] = beta
            psi = nothing
            for d in range(nz):
                xr = crow(d, 0) / (1.0 - psi * crow(d, 2))
                xrp = xr * psi
                red[d, 16:32, :] = xr
                pick("psi", d, psi)
                pick("r2", d, 1.0 / (1.0 - psi * betas[d]))
                pick("wa", d, xrp)
                psi = crow(d, 1) + xrp * crow(d, 0)
            for n, name in enumerate(picks):
                mine[16 * n:16 * n + 16, :] = picks[name]

        psi, r2, beta, r, wa, aw, lam = (mine[16 * n:16 * n + 16, :] for n in range(7))
        A0, W0 = (jnp.concatenate(q, 0) for q in (A, x))
        up_row, down_row = W0 + wa * A0, A0 + aw * W0
        fmine[t, 0], fmine[t, 1] = up_row, down_row
        sends = lev_copies(lambda below: fmine.at[t, below], fgath.at[t], ls_sem.at[t], lr_sem.at[t])
        for c in sends:
            c.start()

        if final:
            def emit(g, carry):
                hvg = at(hv, pl.multiple_of(g * 8, 8))
                for j in range(GROUP):
                    uu, vv = pair(us, g, j), pair(vs, g, j)
                    r0, r1 = roll(uu[0], 1, 0), roll(uu[1], 1, 0)
                    edge = at(hu, 8 + g * 32 + 2 * j + 1, False)
                    put_pair(uo, g, j, (jnp.where(sub < 1, edge, r0), jnp.where(sub < 1, r0, r1)))
                    put_pair(vo, g, j, [
                        jnp.where(
                            lane == 0, roll(hvg, 125 - 4 * (2 * j + m), 1), roll(vv[m], 1, 1)
                        )
                        for m in range(2)
                    ])
                return carry

            each(emit, 0)
        for c in sends:
            c.wait()

        omega = alpha = jnp.zeros((16, 128), F32)
        for d in range(nz - 1):
            omega = jnp.where(me > d, fgath[t, d] + red[d, 16:32, :] * omega, omega)
        for d in range(nz - 1, 0, -1):
            alpha = jnp.where(me < d, fgath[t, d] + red[d, 0:16, :] * alpha, alpha)
        wb = r2 * (omega + psi * (down_row + lam * alpha))
        pa = alpha + beta * (r * (W0 + crow(me, 1) * alpha + crow(me, 0) * wb))
        if final:
            ends[0:16, :], ends[16:32, :] = wb, pa
            break
        wb2, pa2 = (wb[0:8], wb[8:16]), (pa[0:8], pa[8:16])

        def implicit(g, wprev):
            acc = zero
            for j in range(GROUP):
                w0, xx, yy = pair(w, g, j), pair(X, g, j), pair(Y, g, j)
                ss, star = pair(s, g, j), pair(ps, g, j)
                wn = tuple(w0[m] + xx[m] * wb2[m] + yy[m] * pa2[m] for m in range(2))
                pn = tuple(star[m] - ss[m] * (wn[m] - wprev[m]) for m in range(2))
                put_pair(w, g, j, wn)
                put_pair(p, g, j, pn)
                acc = pack_edges(g, j, pn, acc, i_low.at[t + 1], i_high.at[t + 1], 0)
                wprev = wn
            j_own[t + 1, pl.ds(pl.multiple_of(g * 8, 8), 8), :] = acc
            return wprev

        each(implicit, wb2)
        dense(t + 1, False)
        halos = halo_copies(t + 1)
        for c in halos:
            c.start()


def store(u, v, w, ps, X, Y, s, ends, u_out, v_out, w_out, p_out, wo, po, sem):
    rows = w.shape[0] // 4
    copies = [
        pltpu.make_async_copy(src, dst, sem.at[n])
        for n, (src, dst) in enumerate(((u, u_out), (v, v_out)))
    ]
    for c in copies:
        c.start()
    wb, pa = ends[0:16, :], ends[16:32, :]
    wprev = wb
    for part in range(4):
        for l in range(part * rows, (part + 1) * rows, 16):
            wn = w[l:l + 16, :] + X[l:l + 16, :] * wb + Y[l:l + 16, :] * pa
            wo[l:l + 16, :] = wn
            po[l:l + 16, :] = ps[l:l + 16, :] - s[l:l + 16, :] * (wn - wprev)
            wprev = wn
        for n, (src, dst) in enumerate(((wo, w_out), (po, p_out))):
            c = pltpu.make_async_copy(
                src.at[pl.ds(part * rows, rows)], dst.at[pl.ds(part * rows, rows)],
                sem.at[2 + 2 * part + n],
            )
            c.start()
            copies.append(c)
    for c in copies:
        c.wait()


def solution(mesh):
    nx, ny, nz = (mesh.shape[a] for a in ("gx", "gy", "lev"))

    def shards(*fields):
        K, I, J = fields[0].shape
        assert I == 16 and J == 128 and K % (2 * GROUP) == 0
        R, KJ, T = K * I, 8 * (K // GROUP), SUBSTEPS
        full = pltpu.VMEM((R, J), F32)
        ihalo = pltpu.VMEM((T, 6 * K + 16, J), F32)
        jhalo = pltpu.VMEM((T, 3 * KJ, J), F32)
        jdense = pltpu.VMEM((T, KJ, J), F32)
        outs = pl.pallas_call(
            functools.partial(kernel, K, nx, ny, nz),
            out_shape=[full] * 7 + [pltpu.VMEM((32, J), F32)],
            in_specs=[pl.BlockSpec(memory_space=pl.ANY)] * 6,
            out_specs=[pl.BlockSpec(memory_space=pltpu.VMEM)] * 8,
            scratch_shapes=[full] * 9 + [ihalo] * 4 + [jhalo] + [jdense] * 4 + [
                pltpu.VMEM((2 * K + 16, J), F32),
                pltpu.VMEM((2 * K + 16, J), F32),
                pltpu.VMEM((KJ, J), F32),
                pltpu.VMEM((KJ, J), F32),
                pltpu.VMEM((KJ, J), F32),
                pltpu.VMEM((KJ, J), F32),
                pltpu.VMEM((48, J), F32),
                pltpu.VMEM((nz, 48, J), F32),
                pltpu.VMEM((T, 2, 16, J), F32),
                pltpu.VMEM((T, nz, 16, J), F32),
                pltpu.VMEM((nz, 32, J), F32),
                pltpu.VMEM((112, J), F32),
                pltpu.SemaphoreType.DMA((6,)),
                pltpu.SemaphoreType.DMA((T, 4)),
                pltpu.SemaphoreType.DMA((T, 4)),
                pltpu.SemaphoreType.DMA((max(nz - 1, 1),)),
                pltpu.SemaphoreType.DMA((max(nz - 1, 1),)),
                pltpu.SemaphoreType.DMA((T, max(nz - 1, 1))),
                pltpu.SemaphoreType.DMA((T, max(nz - 1, 1))),
            ],
            compiler_params=pltpu.CompilerParams(
                collective_id=0, has_side_effects=True, vmem_limit_bytes=61800 * 1024
            ),
        )(*(f.reshape(R, J) for f in fields))
        outs = pl.pallas_call(
            store,
            out_shape=[jax.ShapeDtypeStruct((R, J), F32)] * 4,
            in_specs=[pl.BlockSpec(memory_space=pltpu.VMEM)] * 8,
            out_specs=[pl.BlockSpec(memory_space=pl.ANY)] * 4,
            scratch_shapes=[full, full, pltpu.SemaphoreType.DMA((10,))],
            compiler_params=pltpu.CompilerParams(vmem_limit_bytes=61800 * 1024),
        )(*(pltpu.with_memory_space_constraint(o, pltpu.VMEM) for o in outs))
        return tuple(o.reshape(K, I, J) for o in outs)

    spec = P("lev", "gx", "gy")
    return jax.shard_map(
        shards, mesh=mesh, in_specs=(spec,) * 6, out_specs=(spec,) * 4, check_vma=False
    )
```
